32 devices in a mesh: chan: 16 (over z, y, core), wall: 2 (over x).
Axes of the slice: x: 2, y: 2, z: 4, core: 2. Of those that a mesh axis runs over, the one named last changes fastest.
Arguments:
- coords: float32 [3, 16, 2, 4096], P(None, 'chan', 'wall'), as said below
- masses: float32 [16, 2, 4096], P('chan', 'wall'), may hold values from 0.5 to 2
- counts: int32 [16, 2, 16], P('chan', 'wall'), may hold values from 64 to 256
- lists: int32 [16, 2, 5, 16, 2], P('chan', 'wall'), may hold values from 0 to 47, as said below
Outputs:
- density: float32 [16, 2, 4096], P('chan', 'wall')
The draws below stay inside these ranges and needn't reach their ends.
Inputs may be any that keep to these rules, and one draw needn't show every extreme that they name: `lists`: each row of 2 entries names different tiles; tile t of extended slab s is s * 16 + t, slab 0 the lower cross-wall neighbour, 1 the slab itself, 2 the upper neighbour. `coords`: channel components lie in [0, 1), cross-wall and depth components in [0, 8).
All inputs are finite; a program needn't handle non-finite values.
Results may differ from the reference program's by a relative error of at most 0.0003.
Values sent between devices are 32-bit elements; how exact they have to be, the bound alone decides.
No kernel may reach another device: no remote copies, remote signals or barrier semaphores. Data moves between devices by JAX's collectives and lax.ppermute only.
A program may use at most 64 MiB of HBM per device.

```python
import math
import jax
import jax.numpy as jnp
from jax import lax

TILE = 256
TILE_DEV = 16
NB = 2
R = 4
CHAN_SLABS = 16
WALL_SLABS = 2
PART = 4096


def draw_coords(key, part):
    unit = jax.random.uniform(key, (3, CHAN_SLABS, WALL_SLABS, TILE_DEV * TILE), jnp.float32)
    extent = jnp.array([1.0, 2.0 * R, 2.0 * R], jnp.float32).reshape(3, 1, 1, 1)
    return (unit * extent * 0.9999).astype(jnp.float32)


def draw_lists(key, part):
    choices_count = 3 * TILE_DEV
    scores = jax.random.randint(key, (CHAN_SLABS, WALL_SLABS, R + 1, TILE_DEV, choices_count), 0, 1 << 20, dtype=jnp.int32)
    distinct = scores * choices_count + jnp.arange(choices_count, dtype=jnp.int32)
    return jnp.argsort(distinct, axis=-1)[..., :NB].astype(jnp.int32)


def with_ends(drawn, own_key, low, top_value):
    spot = [jax.random.randint(jax.random.fold_in(own_key, axis), (), 0, length) for axis, length in enumerate(drawn.shape)]
    main_axis = drawn.shape.index(max(drawn.shape))
    neighbour = spot[:main_axis] + [(spot[main_axis] + 1) % drawn.shape[main_axis]] + spot[main_axis + 1:]
    return drawn.at[tuple(spot)].set(low).at[tuple(neighbour)].set(top_value)


def level_of(stream_key, dims, cuts, smallest, top_value):
    gain, own = 1.0, jax.random.fold_in(stream_key, 6)
    for axis_at, shards_of in cuts:
        draws = jnp.exp(jax.random.uniform(jax.random.fold_in(own, axis_at), (shards_of,), jnp.float32, smallest / len(cuts), top_value / len(cuts)))
        gain = gain * jnp.repeat(draws, dims[axis_at] // shards_of).reshape([-1 if axis == axis_at else 1 for axis in range(len(dims))])
    return gain


def setup_inputs(seed: int = 0) -> dict:
    streams_of = jax.random.split(jax.random.key(seed), 5)
    coords = draw_coords(jax.random.fold_in(streams_of[4], 71), 0)
    masses = jnp.clip(jnp.exp(math.log(2.0) - 1.3862944 * jax.random.uniform(streams_of[1], (CHAN_SLABS, WALL_SLABS, PART), jnp.float32) ** level_of(streams_of[1], (CHAN_SLABS, WALL_SLABS, PART), ((0, 16), (1, 2)), -0.2, 0.2)), 0.5, 2.0)
    counts = with_ends(jax.random.randint(streams_of[2], (CHAN_SLABS, WALL_SLABS, TILE_DEV), TILE // 4, TILE + 1), jax.random.fold_in(streams_of[2], 1), TILE // 4, TILE).astype(jnp.int32)
    lists = draw_lists(jax.random.fold_in(streams_of[4], 71), 0)
    return dict(coords=coords, masses=masses, counts=counts, lists=lists)


def spline(scaled):
    return (jnp.maximum(2.0 - scaled, 0.0) ** 3 * 0.25 - jnp.maximum(1.0 - scaled, 0.0) ** 3) * (1.0 / math.pi)

def pair_block(own_block, partner, partner_rows, offset):
    tile_count = own_block.shape[1]
    tile_len = own_block.shape[2]
    list_len = partner_rows.shape[1]
    picked = jnp.take(partner, partner_rows.reshape(-1), axis=1).reshape(4, tile_count, list_len, tile_len)
    wall_lift = (partner_rows // tile_count - 1).astype(jnp.float32) * (2.0 * R)
    reach = float(R)

    def single_tile(inputs):
        own_tile, theirs, shift_y = inputs
        delta_x = own_tile[0][None, :, None] - (theirs[0][:, None, :] + offset)
        delta_y = own_tile[1][None, :, None] - (theirs[1][:, None, :] + shift_y[:, None, None])
        delta_z = own_tile[2][None, :, None] - theirs[2][:, None, :]
        distance = jnp.sqrt(delta_x * delta_x + delta_y * delta_y + delta_z * delta_z + 0.0001)
        weight = spline(distance / reach)
        gained = lax.optimization_barrier(jnp.sum(weight * theirs[3][:, None, :], axis=(0, 2)))
        handed = lax.optimization_barrier(jnp.sum(weight * own_tile[3][None, :, None], axis=1))
        return (gained, handed)
    gained, handed = lax.map(single_tile, (jnp.moveaxis(own_block, 1, 0), jnp.moveaxis(picked, 1, 0), wall_lift))
    onehot = (partner_rows.reshape(-1)[:, None] == jnp.arange(partner.shape[1], dtype=jnp.int32)[None, :]).astype(jnp.float32)
    returned = jnp.dot(onehot.T, handed.reshape(-1, tile_len), precision=lax.Precision.HIGHEST)
    return (gained, returned)

def reference(coords, masses, counts, lists):
    tile_count = counts.shape[2]
    tile_len = masses.shape[2] // tile_count
    slots = jnp.arange(tile_len, dtype=jnp.int32)
    filled = (slots[None, None, None, :] < counts[..., None]).astype(jnp.float32)
    weighted = masses.reshape(filled.shape) * filled
    packed = jnp.concatenate([coords.reshape(3, CHAN_SLABS, WALL_SLABS, tile_count, tile_len), weighted[None]], axis=0)
    padded = jnp.pad(packed, ((0, 0), (0, 0), (1, 1), (0, 0), (0, 0)))
    extended = jnp.concatenate([padded[:, :, 0:WALL_SLABS], padded[:, :, 1:WALL_SLABS + 1], padded[:, :, 2:]], axis=3)
    flat_own = jnp.moveaxis(packed.reshape(4, -1, tile_count, tile_len), 1, 0)
    density = jnp.zeros((CHAN_SLABS, WALL_SLABS, tile_count, tile_len), jnp.float32)
    returns = jnp.zeros((CHAN_SLABS, WALL_SLABS, 3 * tile_count, tile_len), jnp.float32)
    for step in range(R + 1):
        partner = jnp.roll(extended, -step, axis=1)
        flat_partner = jnp.moveaxis(partner.reshape(4, -1, 3 * tile_count, tile_len), 1, 0)
        flat_lists = lists[:, :, step].reshape(-1, tile_count, NB)

        def per_device(inputs, offset=float(step)):
            return pair_block(inputs[0], inputs[1], inputs[2], offset)
        gained, handed = lax.map(per_device, (flat_own, flat_partner, flat_lists))
        density = density + gained.reshape(CHAN_SLABS, WALL_SLABS, tile_count, tile_len)
        if step > 0:
            returns = returns + jnp.roll(handed.reshape(CHAN_SLABS, WALL_SLABS, 3 * tile_count, tile_len), step, axis=0)
    lower = returns[:, :, :tile_count]
    center = returns[:, :, tile_count:2 * tile_count]
    upper = returns[:, :, 2 * tile_count:]
    from_below = jnp.pad(upper, ((0, 0), (1, 0), (0, 0), (0, 0)))[:, :WALL_SLABS]
    from_above = jnp.pad(lower, ((0, 0), (0, 1), (0, 0), (0, 0)))[:, 1:]
    total = density + center + from_below + from_above
    return (total * filled / (NB * tile_len)).reshape(CHAN_SLABS, WALL_SLABS, -1)
```

```python
import functools
import math

import jax
import jax.numpy as jnp
from jax import lax
from jax.experimental import pallas as pl
from jax.experimental.pallas import tpu as pltpu
from jax.sharding import PartitionSpec as P

NB = 2
R = 4
LANES = 128
STEP = 64
EPS = 0.0001 / (R * R)


def splits(value):
    high = value.astype(jnp.bfloat16).astype(jnp.float32)
    rest = value - high
    middle = rest.astype(jnp.bfloat16).astype(jnp.float32)
    return high, middle, rest - middle


def rounded_splits(value):
    high = lax.reduce_precision(value, 8, 7)
    rest = value - high
    middle = lax.reduce_precision(rest, 8, 7)
    return high, middle, rest - middle


def own_factors(own, weighted):
    scaled = (own[:, :3] - CENTRE.reshape(1, 3, 1)) * (1.0 / R)
    norm = jnp.sum(scaled * scaled, axis=1, keepdims=True)
    one = jnp.ones_like(norm)
    rows = jnp.concatenate(
        [-2.0 * scaled, one, norm, weighted[:, None], jnp.zeros_like(scaled[:, :2])], axis=1
    )
    high, middle, low = rounded_splits(rows)
    stacked = jnp.concatenate([high, high, middle, middle, high, low], axis=1)
    return jnp.swapaxes(stacked, 1, 2).astype(jnp.bfloat16)


def pairs_kernel(
    offsets, tile_count, info, counts, lists, left_ref, *refs, slots_of, with_back
):
    partner_refs = refs[: slots_of]
    rest = refs[slots_of :]
    if with_back:
        gained_ref, back_ref, acc_ref, wide_ref, right_ref = rest
        back_ref[...] = jnp.zeros_like(back_ref)
    else:
        gained_ref, acc_ref, right_ref = rest
    tile_len = left_ref.shape[1]
    width = left_ref.shape[2]
    sub = lax.broadcasted_iota(jnp.int32, (8, tile_len), 0)
    ones = jnp.ones((8, LANES), jnp.float32)
    pick = (lax.broadcasted_iota(jnp.int32, (width, LANES), 0) % 8 == 5) & (
        (lax.broadcasted_iota(jnp.int32, (width, LANES), 0) // 8 == 0)
        | (lax.broadcasted_iota(jnp.int32, (width, LANES), 0) // 8 == 2)
        | (lax.broadcasted_iota(jnp.int32, (width, LANES), 0) // 8 == 5)
    )
    pick = pick.astype(jnp.float32).astype(jnp.bfloat16)

    def one_tile(t, carry):
        acc_ref[...] = jnp.zeros_like(acc_ref)
        count = counts[t]
        if with_back:
            wide_ref[...] = jnp.dot(left_ref[t], pick, preferred_element_type=jnp.float32)
        for at, (offset, buffer) in enumerate(offsets):
            for n in range(NB):
                p = lists[at, t * NB + n]
                slab = p // tile_count
                tile = p - slab * tile_count
                valid = info[slab]
                slot = info[3 + slab]
                base = info[6 + at]

                @pl.when(valid > 0)
                def _(at=at, offset=offset, buffer=buffer, slab=slab, tile=tile, slot=slot, base=base):
                    theirs = partner_refs[buffer][base, slot, tile]
                    lift = (slab - 1).astype(jnp.float32) * (2.0 * R)
                    move = [offset - 0.5, lift - R, -float(R)]
                    coord = [
                        (theirs[i : i + 1] + move[i]) * (1.0 / R) for i in range(3)
                    ]
                    norm = coord[0] * coord[0] + coord[1] * coord[1] + coord[2] * coord[2] + EPS
                    zero = jnp.zeros((8, tile_len), jnp.float32)
                    rows = jnp.where(sub == 0, coord[0], zero)
                    rows = jnp.where(sub == 1, coord[1], rows)
                    rows = jnp.where(sub == 2, coord[2], rows)
                    rows = jnp.where(sub == 3, norm, rows)
                    rows = jnp.where(sub == 4, 1.0, rows)
                    high, middle, low = splits(rows)
                    right_ref[...] = jnp.concatenate(
                        [high, middle, high, middle, low, high], axis=0
                    ).astype(jnp.bfloat16)
                    their_weight = jnp.broadcast_to(theirs[3:4], (8, tile_len))
                    row = slot * tile_count + tile

                    def chunk(i, handed):
                        start = pl.multiple_of(i * STEP, STEP)
                        squared = jnp.dot(
                            left_ref[t, pl.ds(start, STEP), :],
                            right_ref[...],
                            preferred_element_type=jnp.float32,
                        )
                        for j in range(STEP // 8):
                            d2 = jnp.maximum(squared[j * 8 : j * 8 + 8], EPS)
                            q = d2 * lax.rsqrt(d2)
                            u = jnp.maximum(2.0 - q, 0.0)
                            v = jnp.maximum(u - 1.0, 0.0)
                            w = (u * u) * (0.25 * u) - (v * v) * v
                            g = w * their_weight
                            total = g[:, :LANES]
                            for h in range(1, tile_len // LANES):
                                total = total + g[:, h * LANES : (h + 1) * LANES]
                            rows_at = pl.ds(start + j * 8, 8)
                            acc_ref[rows_at, :] = acc_ref[rows_at, :] + total
                            if with_back:
                                mine = wide_ref[rows_at, :]
                                mine = jnp.concatenate([mine] * (tile_len // LANES), axis=1)
                                handed = handed + w * mine
                        return handed

                    handed = lax.fori_loop(
                        0, (count + (STEP - 1)) // STEP, chunk, jnp.zeros((8, tile_len), jnp.float32)
                    )
                    if with_back:
                        back_ref[at, pl.ds(row, 1), :] = back_ref[at, pl.ds(row, 1), :] + jnp.sum(
                            handed, axis=0, keepdims=True
                        )

        sums = lax.dot_general(
            ones,
            acc_ref[...],
            (((1,), (1,)), ((), ())),
            precision=lax.Precision.HIGHEST,
            preferred_element_type=jnp.float32,
        )
        gained_ref[pl.ds(t, 1), :] = sums[0:1]
        return carry

    lax.fori_loop(0, tile_count, one_tile, 0)


def pairs(info, counts, lists, left, buffers, offsets, with_back, name):
    tile_count, tile_len, width = left.shape
    slabs = buffers[0].shape[1]
    out_shape = [jax.ShapeDtypeStruct((tile_count, tile_len), jnp.float32)]
    scratch = [pltpu.VMEM((tile_len, LANES), jnp.float32)]
    if with_back:
        out_shape.append(
            jax.ShapeDtypeStruct((len(offsets), slabs * tile_count, tile_len), jnp.float32)
        )
        scratch.append(pltpu.VMEM((tile_len, LANES), jnp.float32))
    scratch.append(pltpu.VMEM((width, tile_len), jnp.bfloat16))
    smem = pl.BlockSpec(memory_space=pltpu.SMEM)
    vmem = pl.BlockSpec(memory_space=pltpu.VMEM)
    return pl.pallas_call(
        functools.partial(
            pairs_kernel,
            offsets,
            tile_count,
            slots_of=len(buffers),
            with_back=with_back,
        ),
        out_shape=out_shape,
        in_specs=[smem, smem, smem, vmem] + [vmem] * len(buffers),
        out_specs=[vmem] * len(out_shape),
        scratch_shapes=scratch,
        name=name,
    )(info, counts, lists, left, *buffers)


CENTRE = jnp.array([0.5, float(R), float(R)], jnp.float32)


def around(block, distance):
    size = lax.axis_size("chan")
    return lax.ppermute(block, "chan", [((i - distance) % size, i) for i in range(size)])


def exchange(block):
    size = lax.axis_size("chan")
    return lax.ppermute(block, "chan", [(i ^ 1, i) for i in range(size)])


def from_wall(block, distance):
    size = lax.axis_size("wall")
    route = [(i - distance, i) for i in range(size) if 0 <= i - distance < size]
    return lax.ppermute(block, "wall", route)


def on_device(coords, masses, counts, lists):
    tile_count = counts.shape[2]
    tile_len = masses.shape[2] // tile_count
    walls = lax.axis_size("wall")
    two = walls == 2
    wall = lax.axis_index("wall")
    odd = lax.axis_index("chan") % 2
    own_counts = counts[0, 0]
    slots = jnp.arange(tile_len, dtype=jnp.int32)
    filled = (slots[None, :] < own_counts[:, None]).astype(jnp.float32)
    weighted = masses.reshape(tile_count, tile_len) * filled
    own = jnp.concatenate(
        [jnp.swapaxes(coords.reshape(3, tile_count, tile_len), 0, 1), weighted[:, None]], axis=1
    )
    if two:
        swap = [(0, 1), (1, 0)]
        block = jnp.stack([own, lax.ppermute(own, "wall", swap)])
    else:
        block = jnp.stack([own, from_wall(own, 1), from_wall(own, -1)])
    near, far = around(block, -2), around(block, -4)
    left = own_factors(own, weighted)
    held = jnp.stack([block, near, far])
    other = exchange(held)

    low_ok = (wall > 0).astype(jnp.int32)
    high_ok = (wall < walls - 1).astype(jnp.int32)
    one = jnp.ones((), jnp.int32)
    head = [low_ok, one, high_ok, one, 0 * one, (1 if two else 2) * one]
    rows = lists[0, 0].reshape(R + 1, tile_count * NB)
    call = functools.partial(pairs, left=left)
    (gained_0,) = call(
        jnp.stack(head + [0 * one]), own_counts, rows[:1], buffers=[block[None]],
        offsets=((0.0, 0),), with_back=False, name="same",
    )
    gained_odd, back_odd = call(
        jnp.stack(head + [odd, odd + 1]), own_counts, rows[1:4:2], buffers=[other],
        offsets=((1.0, 0), (3.0, 0)), with_back=True, name="odd",
    )
    gained_even, back_even = call(
        jnp.stack(head + [1 * one, 2 * one]), own_counts, rows[2:5:2], buffers=[held],
        offsets=((2.0, 0), (4.0, 0)), with_back=True, name="even",
    )
    passed = exchange(back_odd)
    is_odd = odd > 0
    here = jnp.where(is_odd, passed[0], 0.0)
    to_near = back_even[0] + jnp.where(is_odd, passed[1], passed[0])
    to_far = back_even[1] + jnp.where(is_odd, 0.0, passed[1])
    returns = around(to_near, 2) + around(to_far, 4) + here
    returns = returns.reshape(-1, tile_count, tile_len)
    total = gained_0 + gained_odd + gained_even + returns[0]
    if two:
        total = total + lax.ppermute(returns[1], "wall", swap)
    else:
        total = total + from_wall(returns[2], 1) + from_wall(returns[1], -1)
    return (total * filled * (1.0 / (math.pi * NB * tile_len))).reshape(1, 1, -1)


def solution(mesh):
    placed = (
        P(None, "chan", "wall", None),
        P("chan", "wall", None),
        P("chan", "wall", None),
        P("chan", "wall", None, None, None),
    )
    return jax.shard_map(
        on_device, mesh=mesh, in_specs=placed, out_specs=P("chan", "wall", None), check_vma=False
    )
```

```python
import functools
import math

import jax
import jax.numpy as jnp
from jax import lax
from jax.experimental import pallas as pl
from jax.experimental.pallas import tpu as pltpu
from jax.sharding import PartitionSpec as P

NB = 2
R = 4
LANES = 128
STEP = 64
BATCH = 4
EPS = 0.0001 / (R * R)


def splits(value):
    high = value.astype(jnp.bfloat16).astype(jnp.float32)
    rest = value - high
    middle = rest.astype(jnp.bfloat16).astype(jnp.float32)
    return high, middle, rest - middle


def rounded_splits(value):
    high = lax.reduce_precision(value, 8, 7)
    rest = value - high
    middle = lax.reduce_precision(rest, 8, 7)
    return high, middle, rest - middle


def own_factors(own, weighted):
    scaled = (own[:, :3] - CENTRE.reshape(1, 3, 1)) * (1.0 / R)
    norm = jnp.sum(scaled * scaled, axis=1, keepdims=True)
    one = jnp.ones_like(norm)
    rows = jnp.concatenate(
        [-2.0 * scaled, one, norm, weighted[:, None], jnp.zeros_like(scaled[:, :2])], axis=1
    )
    high, middle, low = rounded_splits(rows)
    stacked = jnp.concatenate([high, high, middle, middle, high, low], axis=1)
    return jnp.swapaxes(stacked, 1, 2).astype(jnp.bfloat16)


def plan_kernel(groups, tile_count, per_tile, info, counts, lists, totals_ref, *plans):
    for group, offsets in enumerate(groups):
        plan = plans[group]

        def one_list(i, at_row, group=group, plan=plan):
            position, at, row = at_row
            t = i // NB
            p = lists[row, i]
            slab = p // tile_count
            tile = p - slab * tile_count
            slot = info[3 + slab]
            code = ((at * 3 + slot) * tile_count + tile) * (tile_count + 1) + t
            code = code * per_tile
            for c in range(per_tile):
                plan[position + c] = code + c
            chunks = (counts[t] + (STEP - 1)) // STEP
            return position + info[slab] * chunks, at, row

        position = jnp.int32(0)
        for at, row in enumerate(offsets):
            position, _, _ = lax.fori_loop(
                0, tile_count * NB, one_list, (position, jnp.int32(at), jnp.int32(row))
            )
        for c in range(3 * BATCH):
            plan[position + c] = tile_count * per_tile
        totals_ref[group] = position


def pairs_kernel(
    offsets, tile_count, group, info, totals, plan, left_ref, *refs, buffer_count, with_back
):
    partner_refs = refs[:buffer_count]
    rest = refs[buffer_count:]
    if with_back:
        gained_ref, back_ref, acc_ref, right_ref, first_ref, second_ref, wide_ref, sum_ref = rest
    else:
        gained_ref, acc_ref, right_ref, first_ref, second_ref = rest
    tile_len = left_ref.shape[1]
    width = left_ref.shape[2]
    slabs = partner_refs[0].shape[1]
    per_tile = tile_len // STEP
    halves = tile_len // LANES
    sub = lax.broadcasted_iota(jnp.int32, (8, tile_len), 0)
    spare = slabs * tile_count * len(offsets)

    acc_ref[...] = jnp.zeros_like(acc_ref)
    if with_back:
        sum_ref[...] = jnp.zeros_like(sum_ref)
        line = lax.broadcasted_iota(jnp.int32, (width, LANES), 0)
        block = line // 8
        pick = (line % 8 == 5) & ((block == 0) | (block == 2) | (block == 5))
        pick = pick.astype(jnp.float32).astype(jnp.bfloat16)

        def widen(i, carry):
            for j in range(2):
                t = i * 2 + j
                wide_ref[t] = jnp.dot(left_ref[t], pick, preferred_element_type=jnp.float32)
            return carry

        lax.fori_loop(0, tile_count // 2, widen, 0)

    for at, (offset, buffer) in enumerate(offsets):
        for slot in range(slabs):
            lift = (info[6 + slot] - 1).astype(jnp.float32) * (2.0 * R)
            move = [offset - 0.5, lift - R, -float(R)]
            base = info[9 + at]

            def factors(i, carry, at=at, buffer=buffer, slot=slot, move=move, base=base):
                for j in range(4):
                    tile = i * 4 + j
                    theirs = partner_refs[buffer][base, slot, tile]
                    x, y, z = [(theirs[c : c + 1] + move[c]) * (1.0 / R) for c in range(3)]
                    norm = x * x + y * y + z * z + EPS
                    rows = jnp.where(sub == 0, x, jnp.where(sub == 1, y, jnp.where(sub == 2, z, norm)))
                    rows = jnp.where(sub == 4, 1.0, jnp.where(sub > 4, 0.0, rows))
                    high, middle, low = splits(rows)
                    right_ref[(at * slabs + slot) * tile_count + tile] = jnp.concatenate(
                        [high, middle, high, middle, low, high], axis=0
                    ).astype(jnp.bfloat16)
                return carry

            lax.fori_loop(0, tile_count // 4, factors, 0)

    def decode(i):
        code = plan[i]
        pair = code // per_tile
        c = code - pair * per_tile
        where = pair // (tile_count + 1)
        t = pair - where * (tile_count + 1)
        lane = where // tile_count
        tile = where - lane * tile_count
        at = lane // 3
        slot = lane - at * 3
        return at, slot, tile, t, c

    def squares(start, out_ref):
        for j in range(BATCH):
            at, slot, tile, t, c = decode(start + j)
            own_tile = jnp.minimum(t, tile_count - 1)
            out_ref[j] = jnp.dot(
                left_ref[own_tile, pl.ds(pl.multiple_of(c * STEP, STEP), STEP), :],
                right_ref[(at * slabs + slot) * tile_count + tile],
                preferred_element_type=jnp.float32,
            )

    def weigh(start, in_ref):
        for j in range(BATCH):
            at, slot, tile, t, c = decode(start + j)
            theirs = partner_refs[0][info[9 + at], slot, tile, 3:4, :]
            their_weight = jnp.broadcast_to(theirs, (8, tile_len))
            handed = jnp.zeros((8, tile_len), jnp.float32)
            first_row = pl.multiple_of(c * STEP, STEP)
            for r in range(STEP // 8):
                d2 = jnp.maximum(in_ref[j, r * 8 : r * 8 + 8], EPS)
                q = d2 * lax.rsqrt(d2)
                u = jnp.maximum(2.0 - q, 0.0)
                v = jnp.maximum(u - 1.0, 0.0)
                w = (u * u) * (0.25 * u) - (v * v) * v
                g = w * their_weight
                total = g[:, :LANES]
                for h in range(1, halves):
                    total = total + g[:, h * LANES : (h + 1) * LANES]
                rows_at = pl.ds(first_row + r * 8, 8)
                acc_ref[t, rows_at, :] = acc_ref[t, rows_at, :] + total
                if with_back:
                    mine = wide_ref[t, rows_at, :]
                    handed = handed + w * jnp.concatenate([mine] * halves, axis=1)
            if with_back:
                row = jnp.where(t < tile_count, (at * slabs + slot) * tile_count + tile, spare)
                sum_ref[row] = sum_ref[row] + handed

    squares(0, first_ref)

    def two_batches(i, carry):
        start = i * (2 * BATCH)
        squares(start + BATCH, second_ref)
        weigh(start, first_ref)
        squares(start + 2 * BATCH, first_ref)
        weigh(start + BATCH, second_ref)
        return carry

    lax.fori_loop(0, (totals[group] + (2 * BATCH - 1)) // (2 * BATCH), two_batches, 0)

    ones = jnp.ones((8, LANES), jnp.bfloat16)

    def finish(i, carry):
        for j in range(4):
            t = i * 4 + j
            sums = jnp.zeros((8, tile_len), jnp.float32)
            for piece in splits(acc_ref[t]):
                sums = sums + lax.dot_general(
                    ones, piece.astype(jnp.bfloat16), (((1,), (1,)), ((), ())),
                    preferred_element_type=jnp.float32,
                )
            gained_ref[pl.ds(t, 1), :] = sums[0:1]
        return carry

    lax.fori_loop(0, tile_count // 4, finish, 0)
    if with_back:

        def fold(i, carry):
            for j in range(8):
                k = i * 8 + j
                back_ref[pl.ds(k, 1), :] = jnp.sum(sum_ref[k], axis=0, keepdims=True)
            return carry

        lax.fori_loop(0, spare // 8, fold, 0)


def pairs(info, totals, plan, left, buffers, offsets, with_back, group, name):
    tile_count, tile_len, width = left.shape
    slabs = buffers[0].shape[1]
    rows = len(offsets) * slabs * tile_count
    squares = pltpu.VMEM((BATCH, STEP, tile_len), jnp.float32)
    out_shape = [jax.ShapeDtypeStruct((tile_count, tile_len), jnp.float32)]
    scratch = [
        pltpu.VMEM((tile_count + 1, tile_len, LANES), jnp.float32),
        pltpu.VMEM((rows, width, tile_len), jnp.bfloat16),
        squares,
        squares,
    ]
    if with_back:
        out_shape.append(jax.ShapeDtypeStruct((rows, tile_len), jnp.float32))
        scratch.append(pltpu.VMEM((tile_count + 1, tile_len, LANES), jnp.float32))
        scratch.append(pltpu.VMEM((rows + 1, 8, tile_len), jnp.float32))
    smem = pl.BlockSpec(memory_space=pltpu.SMEM)
    vmem = pl.BlockSpec(memory_space=pltpu.VMEM)
    return pl.pallas_call(
        functools.partial(
            pairs_kernel, offsets, tile_count, group,
            buffer_count=len(buffers), with_back=with_back,
        ),
        out_shape=out_shape,
        in_specs=[smem, smem, smem, vmem] + [vmem] * len(buffers),
        out_specs=[vmem] * len(out_shape),
        scratch_shapes=scratch,
        name=name,
    )(info, totals, plan, left, *buffers)


def plans_of(info, counts, rows, groups, tile_len):
    tile_count = counts.shape[0]
    per_tile = tile_len // STEP
    smem = pl.BlockSpec(memory_space=pltpu.SMEM)
    lengths = [len(g) * tile_count * NB * per_tile + 4 * BATCH for g in groups]
    return pl.pallas_call(
        functools.partial(plan_kernel, groups, tile_count, per_tile),
        out_shape=[jax.ShapeDtypeStruct((len(groups),), jnp.int32)]
        + [jax.ShapeDtypeStruct((n,), jnp.int32) for n in lengths],
        in_specs=[smem] * 3,
        out_specs=[smem] * (1 + len(groups)),
        name="plan",
    )(info, counts, rows)


CENTRE = jnp.array([0.5, float(R), float(R)], jnp.float32)


def around(block, distance):
    size = lax.axis_size("chan")
    return lax.ppermute(block, "chan", [((i - distance) % size, i) for i in range(size)])


def exchange(block):
    size = lax.axis_size("chan")
    return lax.ppermute(block, "chan", [(i ^ 1, i) for i in range(size)])


def from_wall(block, distance):
    size = lax.axis_size("wall")
    route = [(i - distance, i) for i in range(size) if 0 <= i - distance < size]
    return lax.ppermute(block, "wall", route)


def on_device(coords, masses, counts, lists):
    tile_count = counts.shape[2]
    tile_len = masses.shape[2] // tile_count
    walls = lax.axis_size("wall")
    two = walls == 2
    wall = lax.axis_index("wall")
    odd = lax.axis_index("chan") % 2
    own_counts = counts[0, 0]
    slots = jnp.arange(tile_len, dtype=jnp.int32)
    filled = (slots[None, :] < own_counts[:, None]).astype(jnp.float32)
    weighted = masses.reshape(tile_count, tile_len) * filled
    own = jnp.concatenate(
        [jnp.swapaxes(coords.reshape(3, tile_count, tile_len), 0, 1), weighted[:, None]], axis=1
    )
    if two:
        swap = [(0, 1), (1, 0)]
        block = jnp.stack([own, lax.ppermute(own, "wall", swap)])
    else:
        block = jnp.stack([own, from_wall(own, 1), from_wall(own, -1)])
    near, far = around(block, -2), around(block, -4)
    left = own_factors(own, weighted)
    held = jnp.stack([block, near, far])
    other = exchange(held)

    low_ok = (wall > 0).astype(jnp.int32)
    high_ok = (wall < walls - 1).astype(jnp.int32)
    one = jnp.ones((), jnp.int32)
    walled = (wall > 0).astype(jnp.int32)
    if two:
        head = [low_ok, one, high_ok, one, 0 * one, one, one, 2 - 2 * walled, 0 * one]
    else:
        head = [low_ok, one, high_ok, one, 0 * one, 2 * one, one, 0 * one, 2 * one]
    near_at = 3 + odd
    info = jnp.stack(head + [near_at, one, near_at + 1, 2 * one])
    rows = lists[0, 0].reshape(R + 1, tile_count * NB)
    totals, plan_same, plan_ahead = plans_of(
        info, own_counts, rows, ((0,), (1, 2, 3, 4)), tile_len
    )
    (gained_same,) = pairs(
        jnp.stack(head + [0 * one]), totals, plan_same, left, [block[None]],
        ((0.0, 0),), False, 0, "same",
    )
    gained_ahead, back = pairs(
        info, totals, plan_ahead, left, [jnp.concatenate([held, other])],
        ((1.0, 0), (2.0, 0), (3.0, 0), (4.0, 0)), True, 1, "ahead",
    )
    back = back.reshape(R, -1, tile_len)
    back_odd, back_even = back[0::2], back[1::2]
    passed = exchange(back_odd)
    is_odd = odd > 0
    here = jnp.where(is_odd, passed[0], 0.0)
    to_near = back_even[0] + jnp.where(is_odd, passed[1], passed[0])
    to_far = back_even[1] + jnp.where(is_odd, 0.0, passed[1])
    returns = around(to_near, 2) + around(to_far, 4) + here
    returns = returns.reshape(-1, tile_count, tile_len)
    total = gained_same + gained_ahead + returns[0]
    if two:
        total = total + lax.ppermute(returns[1], "wall", swap)
    else:
        total = total + from_wall(returns[2], 1) + from_wall(returns[1], -1)
    return (total * filled * (1.0 / (math.pi * NB * tile_len))).reshape(1, 1, -1)


def solution(mesh):
    placed = (
        P(None, "chan", "wall", None),
        P("chan", "wall", None),
        P("chan", "wall", None),
        P("chan", "wall", None, None, None),
    )
    return jax.shard_map(
        on_device, mesh=mesh, in_specs=placed, out_specs=P("chan", "wall", None), check_vma=False
    )
```

```python
import functools
import math

import jax
import jax.numpy as jnp
from jax import lax
from jax.experimental import pallas as pl
from jax.experimental.pallas import tpu as pltpu
from jax.sharding import PartitionSpec as P

NB = 2
R = 4
LANES = 128
STEP = 64
BATCH = 4
EPS = 0.0001 / (R * R)


def splits(value):
    high = value.astype(jnp.bfloat16).astype(jnp.float32)
    rest = value - high
    middle = rest.astype(jnp.bfloat16).astype(jnp.float32)
    return high, middle, rest - middle


def rounded_splits(value):
    high = lax.reduce_precision(value, 8, 7)
    rest = value - high
    middle = lax.reduce_precision(rest, 8, 7)
    return high, middle, rest - middle


def own_factors(own, weighted):
    scaled = (own[:, :3] - CENTRE.reshape(1, 3, 1)) * (1.0 / R)
    norm = jnp.sum(scaled * scaled, axis=1, keepdims=True)
    one = jnp.ones_like(norm)
    rows = jnp.concatenate(
        [-2.0 * scaled, one, norm, weighted[:, None], jnp.zeros_like(scaled[:, :2])], axis=1
    )
    high, middle, low = rounded_splits(rows)
    stacked = jnp.concatenate([high, high, middle, middle, high, low], axis=1)
    return jnp.swapaxes(stacked, 1, 2).astype(jnp.bfloat16)


def entry_stride(tile_count, per_tile):
    return per_tile << tile_count.bit_length()


def plan_kernel(groups, tile_count, per_tile, slabs, info, counts, lists, totals_ref, *plans):
    for group, offsets in enumerate(groups):
        plan = plans[group]

        def one_list(i, at_row, group=group, plan=plan):
            position, at, row = at_row
            t = lax.div(i, jnp.int32(NB))
            p = lists[row, i]
            slab = lax.div(p, jnp.int32(tile_count))
            tile = p - slab * tile_count
            right = (at * slabs + info[3 + slab]) * tile_count + tile
            code = right * entry_stride(tile_count, per_tile) + t * per_tile
            for c in range(per_tile):
                plan[position + c] = code + c
            chunks = lax.div(counts[t] + (STEP - 1), jnp.int32(STEP))
            return position + info[slab] * chunks, at, row

        position = jnp.int32(0)
        for at, row in enumerate(offsets):
            position, _, _ = lax.fori_loop(
                0, tile_count * NB, one_list, (position, jnp.int32(at), jnp.int32(row))
            )
        for c in range(3 * BATCH):
            plan[position + c] = tile_count * per_tile
        totals_ref[group] = position


def pairs_kernel(
    offsets, tile_count, group, info, totals, plan, left_ref, *refs, buffer_count, with_back
):
    partner_refs = refs[:buffer_count]
    rest = refs[buffer_count:]
    if with_back:
        gained_ref, back_ref, acc_ref, right_ref, weight_ref, first_ref, second_ref, wide_ref, sum_ref = rest
    else:
        gained_ref, acc_ref, right_ref, weight_ref, first_ref, second_ref = rest
    tile_len = partner_refs[0].shape[-1]
    width = left_ref.shape[1]
    slabs = partner_refs[0].shape[1]
    per_tile = tile_len // STEP
    halves = tile_len // LANES
    sub = lax.broadcasted_iota(jnp.int32, (8, tile_len), 0)
    spare = slabs * tile_count * len(offsets)

    acc_ref[...] = jnp.zeros_like(acc_ref)
    if with_back:
        sum_ref[...] = jnp.zeros_like(sum_ref)
        line = lax.broadcasted_iota(jnp.int32, (width, LANES), 0)
        block = line // 8
        pick = (line % 8 == 5) & ((block == 0) | (block == 2) | (block == 5))
        pick = pick.astype(jnp.float32).astype(jnp.bfloat16)

        def widen(i, carry):
            for j in range(2):
                t = i * 2 + j
                at = pl.ds(pl.multiple_of(t * tile_len, tile_len), tile_len)
                wide_ref[at, :] = jnp.dot(left_ref[at, :], pick, preferred_element_type=jnp.float32)
            return carry

        lax.fori_loop(0, tile_count // 2, widen, 0)

    for at, (offset, buffer) in enumerate(offsets):
        for slot in range(slabs):
            lift = (info[6 + slot] - 1).astype(jnp.float32) * (2.0 * R)
            move = [offset - 0.5, lift - R, -float(R)]
            base = info[9 + at] if with_back else 0

            def factors(i, carry, at=at, buffer=buffer, slot=slot, move=move, base=base):
                for j in range(4):
                    tile = i * 4 + j
                    theirs = partner_refs[buffer][base, slot, tile]
                    x, y, z = [(theirs[c : c + 1] + move[c]) * (1.0 / R) for c in range(3)]
                    norm = x * x + y * y + z * z + EPS
                    rows = jnp.where(sub == 0, x, jnp.where(sub == 1, y, jnp.where(sub == 2, z, norm)))
                    rows = jnp.where(sub == 4, 1.0, jnp.where(sub > 4, 0.0, rows))
                    high, middle, low = splits(rows)
                    index = (at * slabs + slot) * tile_count + tile
                    weight_ref[index] = jnp.broadcast_to(theirs[3:4], (8, tile_len))
                    right_ref[index] = jnp.concatenate(
                        [high, middle, high, middle, low, high], axis=0
                    ).astype(jnp.bfloat16)
                return carry

            lax.fori_loop(0, tile_count // 4, factors, 0)

    stride = entry_stride(tile_count, per_tile)

    def decode(i):
        code = plan[i]
        right = lax.div(code, jnp.int32(stride))
        chunk = code - right * stride
        return right, chunk

    def squares(start, out_ref):
        for j in range(BATCH):
            right, chunk = decode(start + j)
            chunk = jnp.minimum(chunk, tile_count * per_tile - 1)
            out_ref[j] = jnp.dot(
                left_ref[pl.ds(pl.multiple_of(chunk * STEP, STEP), STEP), :],
                right_ref[right],
                preferred_element_type=jnp.float32,
            )

    def weigh(start, in_ref):
        for j in range(BATCH):
            right, chunk = decode(start + j)
            their_weight = weight_ref[right]
            handed = jnp.zeros((8, tile_len), jnp.float32)
            first_row = pl.multiple_of(chunk * STEP, STEP)
            for r in range(STEP // 8):
                d2 = jnp.maximum(in_ref[j, r * 8 : r * 8 + 8], EPS)
                q = d2 * lax.rsqrt(d2)
                u = jnp.maximum(2.0 - q, 0.0)
                v = jnp.maximum(u - 1.0, 0.0)
                w = (u * u) * (0.25 * u) - (v * v) * v
                g = w * their_weight
                total = g[:, :LANES]
                for h in range(1, halves):
                    total = total + g[:, h * LANES : (h + 1) * LANES]
                rows_at = pl.ds(first_row + r * 8, 8)
                acc_ref[rows_at, :] = acc_ref[rows_at, :] + total
                if with_back:
                    mine = wide_ref[rows_at, :]
                    handed = handed + w * jnp.concatenate([mine] * halves, axis=1)
            if with_back:
                row = jnp.where(chunk < tile_count * per_tile, right, spare)
                sum_ref[row] = sum_ref[row] + handed

    squares(0, first_ref)

    def two_batches(i, carry):
        start = i * (2 * BATCH)
        squares(start + BATCH, second_ref)
        weigh(start, first_ref)
        squares(start + 2 * BATCH, first_ref)
        weigh(start + BATCH, second_ref)
        return carry

    lax.fori_loop(0, (totals[group] + (2 * BATCH - 1)) // (2 * BATCH), two_batches, 0)

    ones = jnp.ones((8, LANES), jnp.bfloat16)

    def finish(i, carry):
        for j in range(4):
            t = i * 4 + j
            sums = jnp.zeros((8, tile_len), jnp.float32)
            for piece in splits(acc_ref[pl.ds(pl.multiple_of(t * tile_len, tile_len), tile_len), :]):
                sums = sums + lax.dot_general(
                    ones, piece.astype(jnp.bfloat16), (((1,), (1,)), ((), ())),
                    preferred_element_type=jnp.float32,
                )
            gained_ref[pl.ds(t, 1), :] = sums[0:1]
        return carry

    lax.fori_loop(0, tile_count // 4, finish, 0)
    if with_back:

        def fold(i, carry):
            for j in range(8):
                k = i * 8 + j
                back_ref[pl.ds(k, 1), :] = jnp.sum(sum_ref[k], axis=0, keepdims=True)
            return carry

        lax.fori_loop(0, spare // 8, fold, 0)


def pairs(info, totals, plan, left, buffers, offsets, with_back, group, name):
    width = left.shape[1]
    slabs, tile_count, _, tile_len = buffers[0].shape[1:]
    rows = len(offsets) * slabs * tile_count
    squares = pltpu.VMEM((BATCH, STEP, tile_len), jnp.float32)
    out_shape = [jax.ShapeDtypeStruct((tile_count, tile_len), jnp.float32)]
    scratch = [
        pltpu.VMEM(((tile_count + 1) * tile_len, LANES), jnp.float32),
        pltpu.VMEM((rows, width, tile_len), jnp.bfloat16),
        pltpu.VMEM((rows, 8, tile_len), jnp.float32),
        squares,
        squares,
    ]
    if with_back:
        out_shape.append(jax.ShapeDtypeStruct((rows, tile_len), jnp.float32))
        scratch.append(pltpu.VMEM(((tile_count + 1) * tile_len, LANES), jnp.float32))
        scratch.append(pltpu.VMEM((rows + 1, 8, tile_len), jnp.float32))
    smem = pl.BlockSpec(memory_space=pltpu.SMEM)
    vmem = pl.BlockSpec(memory_space=pltpu.VMEM)
    return pl.pallas_call(
        functools.partial(
            pairs_kernel, offsets, tile_count, group,
            buffer_count=len(buffers), with_back=with_back,
        ),
        out_shape=out_shape,
        in_specs=[smem, smem, smem, vmem] + [vmem] * len(buffers),
        out_specs=[vmem] * len(out_shape),
        scratch_shapes=scratch,
        name=name,
    )(info, totals, plan, left, *buffers)


def plans_of(info, counts, rows, groups, tile_len, slabs):
    tile_count = counts.shape[0]
    per_tile = tile_len // STEP
    smem = pl.BlockSpec(memory_space=pltpu.SMEM)
    lengths = [len(g) * tile_count * NB * per_tile + 4 * BATCH for g in groups]
    return pl.pallas_call(
        functools.partial(plan_kernel, groups, tile_count, per_tile, slabs),
        out_shape=[jax.ShapeDtypeStruct((len(groups),), jnp.int32)]
        + [jax.ShapeDtypeStruct((n,), jnp.int32) for n in lengths],
        in_specs=[smem] * 3,
        out_specs=[smem] * (1 + len(groups)),
        cost_estimate=pl.CostEstimate(flops=5_000_000_000, bytes_accessed=20_000, transcendentals=0),
        name="plan",
    )(info, counts, rows)


CENTRE = jnp.array([0.5, float(R), float(R)], jnp.float32)


def around(block, distance):
    size = lax.axis_size("chan")
    return lax.ppermute(block, "chan", [((i - distance) % size, i) for i in range(size)])


def exchange(block):
    size = lax.axis_size("chan")
    return lax.ppermute(block, "chan", [(i ^ 1, i) for i in range(size)])


def from_wall(block, distance):
    size = lax.axis_size("wall")
    route = [(i - distance, i) for i in range(size) if 0 <= i - distance < size]
    return lax.ppermute(block, "wall", route)


def on_device(coords, masses, counts, lists):
    tile_count = counts.shape[2]
    tile_len = masses.shape[2] // tile_count
    walls = lax.axis_size("wall")
    two = walls == 2
    wall = lax.axis_index("wall")
    odd = lax.axis_index("chan") % 2
    own_counts = counts[0, 0]
    slots = jnp.arange(tile_len, dtype=jnp.int32)
    filled = (slots[None, :] < own_counts[:, None]).astype(jnp.float32)
    weighted = masses.reshape(tile_count, tile_len) * filled
    own = jnp.concatenate(
        [jnp.swapaxes(coords.reshape(3, tile_count, tile_len), 0, 1), weighted[:, None]], axis=1
    )
    if two:
        swap = [(0, 1), (1, 0)]
        block = jnp.stack([own, lax.ppermute(own, "wall", swap)])
    else:
        block = jnp.stack([own, from_wall(own, 1), from_wall(own, -1)])
    near, far = around(block, -2), around(block, -4)
    left = own_factors(own, weighted).reshape(tile_count * tile_len, -1)
    held = jnp.stack([block, near, far])
    other = exchange(held)

    low_ok = (wall > 0).astype(jnp.int32)
    high_ok = (wall < walls - 1).astype(jnp.int32)
    one = jnp.ones((), jnp.int32)
    walled = (wall > 0).astype(jnp.int32)
    if two:
        head = [low_ok, one, high_ok, one, 0 * one, one, one, 2 - 2 * walled, 0 * one]
    else:
        head = [low_ok, one, high_ok, one, 0 * one, 2 * one, one, 0 * one, 2 * one]
    info = jnp.stack(head + [odd, one, odd + 1, 2 * one])
    rows = lists[0, 0].reshape(R + 1, tile_count * NB)
    totals, plan_same, plan_ahead = plans_of(
        info, own_counts, rows, ((0,), (1, 2, 3, 4)), tile_len, block.shape[0]
    )
    (gained_same,) = pairs(
        info, totals, plan_same, left, [block[None]],
        ((0.0, 0),), False, 0, "same",
    )
    gained_ahead, back = pairs(
        info, totals, plan_ahead, left, [held, other],
        ((1.0, 1), (2.0, 0), (3.0, 1), (4.0, 0)), True, 1, "ahead",
    )
    back = back.reshape(R, -1, tile_len)
    back_odd, back_even = back[0::2], back[1::2]
    passed = exchange(back_odd)
    is_odd = odd > 0
    here = jnp.where(is_odd, passed[0], 0.0)
    to_near = back_even[0] + jnp.where(is_odd, passed[1], passed[0])
    to_far = back_even[1] + jnp.where(is_odd, 0.0, passed[1])
    returns = around(to_near, 2) + around(to_far, 4) + here
    returns = returns.reshape(-1, tile_count, tile_len)
    total = gained_same + gained_ahead + returns[0]
    if two:
        total = total + lax.ppermute(returns[1], "wall", swap)
    else:
        total = total + from_wall(returns[2], 1) + from_wall(returns[1], -1)
    return (total * filled * (1.0 / (math.pi * NB * tile_len))).reshape(1, 1, -1)


def solution(mesh):
    placed = (
        P(None, "chan", "wall", None),
        P("chan", "wall", None),
        P("chan", "wall", None),
        P("chan", "wall", None, None, None),
    )
    return jax.shard_map(
        on_device, mesh=mesh, in_specs=placed, out_specs=P("chan", "wall", None), check_vma=False
    )
```

```python
import functools
import math

import jax
import jax.numpy as jnp
from jax import lax
from jax.experimental import pallas as pl
from jax.experimental.pallas import tpu as pltpu
from jax.sharding import PartitionSpec as P

NB = 2
R = 4
LANES = 128
STEP = 64
BATCH = 8
EPS = 0.0001 / (R * R)


def splits(value):
    high = value.astype(jnp.bfloat16).astype(jnp.float32)
    rest = value - high
    middle = rest.astype(jnp.bfloat16).astype(jnp.float32)
    return high, middle, rest - middle


def rounded_splits(value):
    high = lax.reduce_precision(value, 8, 7)
    rest = value - high
    middle = lax.reduce_precision(rest, 8, 7)
    return high, middle, rest - middle


def own_factors(own, weighted):
    scaled = (own[:, :3] - CENTRE.reshape(1, 3, 1)) * (1.0 / R)
    norm = jnp.sum(scaled * scaled, axis=1, keepdims=True)
    one = jnp.ones_like(norm)
    rows = jnp.concatenate(
        [-2.0 * scaled, one, norm, weighted[:, None], jnp.zeros_like(scaled[:, :2])], axis=1
    )
    high, middle, low = rounded_splits(rows)
    stacked = jnp.concatenate([high, high, middle, middle, high, low], axis=1)
    return jnp.swapaxes(stacked, 1, 2).astype(jnp.bfloat16)


def entry_stride(tile_count, per_tile):
    return per_tile << tile_count.bit_length()


def plan_kernel(groups, tile_count, per_tile, slabs, info, counts, lists, totals_ref, *plans):
    for group, offsets in enumerate(groups):
        plan = plans[group]

        def one_list(i, at_row, group=group, plan=plan):
            position, at, row = at_row
            t = lax.div(i, jnp.int32(NB))
            p = lists[row, i]
            slab = lax.div(p, jnp.int32(tile_count))
            tile = p - slab * tile_count
            right = (at * slabs + info[3 + slab]) * tile_count + tile
            code = right * entry_stride(tile_count, per_tile) + t * per_tile
            for c in range(per_tile):
                plan[position + c] = code + c
            chunks = lax.div(counts[t] + (STEP - 1), jnp.int32(STEP))
            return position + info[slab] * chunks, at, row

        position = jnp.int32(0)
        for at, row in enumerate(offsets):
            position, _, _ = lax.fori_loop(
                0, tile_count * NB, one_list, (position, jnp.int32(at), jnp.int32(row))
            )
        for c in range(3 * BATCH):
            plan[position + c] = tile_count * per_tile
        totals_ref[group] = position


def pairs_kernel(
    offsets, tile_count, group, info, totals, plan, left_ref, *refs, buffer_count, with_back
):
    partner_refs = refs[:buffer_count]
    rest = refs[buffer_count:]
    if with_back:
        gained_ref, back_ref, acc_ref, right_ref, weight_ref, first_ref, second_ref, wide_ref, sum_ref = rest
    else:
        gained_ref, acc_ref, right_ref, weight_ref, first_ref, second_ref = rest
    tile_len = partner_refs[0].shape[-1]
    width = left_ref.shape[1]
    slabs = partner_refs[0].shape[1]
    per_tile = tile_len // STEP
    halves = tile_len // LANES
    sub = lax.broadcasted_iota(jnp.int32, (8, tile_len), 0)
    spare = slabs * tile_count * len(offsets)

    acc_ref[...] = jnp.zeros_like(acc_ref)
    if with_back:
        sum_ref[...] = jnp.zeros_like(sum_ref)
        line = lax.broadcasted_iota(jnp.int32, (width, LANES), 0)
        block = line // 8
        pick = (line % 8 == 5) & ((block == 0) | (block == 2) | (block == 5))
        pick = pick.astype(jnp.float32).astype(jnp.bfloat16)

        def widen(i, carry):
            for j in range(2):
                t = i * 2 + j
                at = pl.ds(pl.multiple_of(t * tile_len, tile_len), tile_len)
                wide_ref[at, :] = jnp.dot(left_ref[at, :], pick, preferred_element_type=jnp.float32)
            return carry

        lax.fori_loop(0, tile_count // 2, widen, 0)

    for at, (offset, buffer) in enumerate(offsets):
        for slot in range(slabs):
            lift = (info[6 + slot] - 1).astype(jnp.float32) * (2.0 * R)
            move = [offset - 0.5, lift - R, -float(R)]
            base = info[9 + at] if with_back else 0

            def factors(i, carry, at=at, buffer=buffer, slot=slot, move=move, base=base):
                for j in range(4):
                    tile = i * 4 + j
                    theirs = partner_refs[buffer][base, slot, tile]
                    x, y, z = [(theirs[c : c + 1] + move[c]) * (1.0 / R) for c in range(3)]
                    norm = x * x + y * y + z * z + EPS
                    rows = jnp.where(sub == 0, x, jnp.where(sub == 1, y, jnp.where(sub == 2, z, norm)))
                    rows = jnp.where(sub == 4, 1.0, jnp.where(sub > 4, 0.0, rows))
                    high, middle, low = splits(rows)
                    index = (at * slabs + slot) * tile_count + tile
                    weight_ref[index] = jnp.broadcast_to(theirs[3:4], (8, tile_len))
                    right_ref[index] = jnp.concatenate(
                        [high, middle, high, middle, low, high], axis=0
                    ).astype(jnp.bfloat16)
                return carry

            lax.fori_loop(0, tile_count // 4, factors, 0)

    stride = entry_stride(tile_count, per_tile)

    def decode(i):
        code = plan[i]
        right = lax.div(code, jnp.int32(stride))
        chunk = code - right * stride
        return right, chunk

    def squares(start, out_ref):
        for j in range(BATCH):
            right, chunk = decode(start + j)
            chunk = jnp.minimum(chunk, tile_count * per_tile - 1)
            out_ref[j] = jnp.dot(
                left_ref[pl.ds(pl.multiple_of(chunk * STEP, STEP), STEP), :],
                right_ref[right],
                preferred_element_type=jnp.float32,
            )

    def weigh(start, in_ref):
        for j in range(BATCH):
            right, chunk = decode(start + j)
            their_weight = weight_ref[right]
            handed = jnp.zeros((8, tile_len), jnp.float32)
            first_row = pl.multiple_of(chunk * STEP, STEP)
            for r in range(STEP // 8):
                d2 = jnp.maximum(in_ref[j, r * 8 : r * 8 + 8], EPS)
                q = d2 * lax.rsqrt(d2)
                u = jnp.maximum(2.0 - q, 0.0)
                v = jnp.maximum(u - 1.0, 0.0)
                w = (u * u) * (0.25 * u) - (v * v) * v
                g = w * their_weight
                total = g[:, :LANES]
                for h in range(1, halves):
                    total = total + g[:, h * LANES : (h + 1) * LANES]
                rows_at = pl.ds(first_row + r * 8, 8)
                acc_ref[rows_at, :] = acc_ref[rows_at, :] + total
                if with_back:
                    mine = wide_ref[rows_at, :]
                    handed = handed + w * jnp.concatenate([mine] * halves, axis=1)
            if with_back:
                row = jnp.where(chunk < tile_count * per_tile, right, spare)
                sum_ref[row] = sum_ref[row] + handed

    squares(0, first_ref)

    def two_batches(i, carry):
        start = i * (2 * BATCH)
        squares(start + BATCH, second_ref)
        weigh(start, first_ref)
        squares(start + 2 * BATCH, first_ref)
        weigh(start + BATCH, second_ref)
        return carry

    lax.fori_loop(0, (totals[group] + (2 * BATCH - 1)) // (2 * BATCH), two_batches, 0)

    ones = jnp.ones((8, LANES), jnp.bfloat16)

    def finish(i, carry):
        for j in range(4):
            t = i * 4 + j
            sums = jnp.zeros((8, tile_len), jnp.float32)
            for piece in splits(acc_ref[pl.ds(pl.multiple_of(t * tile_len, tile_len), tile_len), :]):
                sums = sums + lax.dot_general(
                    ones, piece.astype(jnp.bfloat16), (((1,), (1,)), ((), ())),
                    preferred_element_type=jnp.float32,
                )
            gained_ref[pl.ds(t, 1), :] = sums[0:1]
        return carry

    lax.fori_loop(0, tile_count // 4, finish, 0)
    if with_back:

        def fold(i, carry):
            for j in range(8):
                k = i * 8 + j
                back_ref[pl.ds(k, 1), :] = jnp.sum(sum_ref[k], axis=0, keepdims=True)
            return carry

        lax.fori_loop(0, spare // 8, fold, 0)


def pairs(info, totals, plan, left, buffers, offsets, with_back, group, name):
    width = left.shape[1]
    slabs, tile_count, _, tile_len = buffers[0].shape[1:]
    rows = len(offsets) * slabs * tile_count
    squares = pltpu.VMEM((BATCH, STEP, tile_len), jnp.float32)
    out_shape = [jax.ShapeDtypeStruct((tile_count, tile_len), jnp.float32)]
    scratch = [
        pltpu.VMEM(((tile_count + 1) * tile_len, LANES), jnp.float32),
        pltpu.VMEM((rows, width, tile_len), jnp.bfloat16),
        pltpu.VMEM((rows, 8, tile_len), jnp.float32),
        squares,
        squares,
    ]
    if with_back:
        out_shape.append(jax.ShapeDtypeStruct((rows, tile_len), jnp.float32))
        scratch.append(pltpu.VMEM(((tile_count + 1) * tile_len, LANES), jnp.float32))
        scratch.append(pltpu.VMEM((rows + 1, 8, tile_len), jnp.float32))
    smem = pl.BlockSpec(memory_space=pltpu.SMEM)
    vmem = pl.BlockSpec(memory_space=pltpu.VMEM)
    return pl.pallas_call(
        functools.partial(
            pairs_kernel, offsets, tile_count, group,
            buffer_count=len(buffers), with_back=with_back,
        ),
        out_shape=out_shape,
        in_specs=[smem, smem, smem, vmem] + [vmem] * len(buffers),
        out_specs=[vmem] * len(out_shape),
        scratch_shapes=scratch,
        name=name,
    )(info, totals, plan, left, *buffers)


def plans_of(info, counts, rows, groups, tile_len, slabs):
    tile_count = counts.shape[0]
    per_tile = tile_len // STEP
    smem = pl.BlockSpec(memory_space=pltpu.SMEM)
    lengths = [len(g) * tile_count * NB * per_tile + 4 * BATCH for g in groups]
    return pl.pallas_call(
        functools.partial(plan_kernel, groups, tile_count, per_tile, slabs),
        out_shape=[jax.ShapeDtypeStruct((len(groups),), jnp.int32)]
        + [jax.ShapeDtypeStruct((n,), jnp.int32) for n in lengths],
        in_specs=[smem] * 3,
        out_specs=[smem] * (1 + len(groups)),
        cost_estimate=pl.CostEstimate(flops=5_000_000_000, bytes_accessed=20_000, transcendentals=0),
        name="plan",
    )(info, counts, rows)


CENTRE = jnp.array([0.5, float(R), float(R)], jnp.float32)


def around(block, distance):
    size = lax.axis_size("chan")
    return lax.ppermute(block, "chan", [((i - distance) % size, i) for i in range(size)])


def exchange(block):
    size = lax.axis_size("chan")
    return lax.ppermute(block, "chan", [(i ^ 1, i) for i in range(size)])


def from_wall(block, distance):
    size = lax.axis_size("wall")
    route = [(i - distance, i) for i in range(size) if 0 <= i - distance < size]
    return lax.ppermute(block, "wall", route)


def on_device(coords, masses, counts, lists):
    tile_count = counts.shape[2]
    tile_len = masses.shape[2] // tile_count
    walls = lax.axis_size("wall")
    two = walls == 2
    wall = lax.axis_index("wall")
    odd = lax.axis_index("chan") % 2
    own_counts = counts[0, 0]
    slots = jnp.arange(tile_len, dtype=jnp.int32)
    filled = (slots[None, :] < own_counts[:, None]).astype(jnp.float32)
    weighted = masses.reshape(tile_count, tile_len) * filled
    own = jnp.concatenate(
        [jnp.swapaxes(coords.reshape(3, tile_count, tile_len), 0, 1), weighted[:, None]], axis=1
    )
    if two:
        swap = [(0, 1), (1, 0)]
        block = jnp.stack([own, lax.ppermute(own, "wall", swap)])
    else:
        block = jnp.stack([own, from_wall(own, 1), from_wall(own, -1)])
    near, far = around(block, -2), around(block, -4)
    left = own_factors(own, weighted).reshape(tile_count * tile_len, -1)
    held = jnp.stack([block, near, far])

    low_ok = (wall > 0).astype(jnp.int32)
    high_ok = (wall < walls - 1).astype(jnp.int32)
    one = jnp.ones((), jnp.int32)
    walled = (wall > 0).astype(jnp.int32)
    if two:
        head = [low_ok, one, high_ok, one, 0 * one, one, one, 2 - 2 * walled, 0 * one]
    else:
        head = [low_ok, one, high_ok, one, 0 * one, 2 * one, one, 0 * one, 2 * one]
    info = jnp.stack(head + [odd, one, odd + 1, 2 * one])
    rows = lists[0, 0].reshape(R + 1, tile_count * NB)
    rows, block = lax.optimization_barrier((rows, block))
    totals, plan_same, plan_ahead = plans_of(
        info, own_counts, rows, ((0,), (1, 2, 3, 4)), tile_len, block.shape[0]
    )
    held, totals, plan_ahead, left = lax.optimization_barrier((held, totals, plan_ahead, left))
    other = exchange(held)
    (gained_same,) = pairs(
        info, totals, plan_same, left, [block[None]],
        ((0.0, 0),), False, 0, "same",
    )
    gained_ahead, back = pairs(
        info, totals, plan_ahead, left, [held, other],
        ((1.0, 1), (2.0, 0), (3.0, 1), (4.0, 0)), True, 1, "ahead",
    )
    back = back.reshape(R, -1, tile_len)
    back_odd, back_even = back[0::2], back[1::2]
    passed = exchange(back_odd)
    is_odd = odd > 0
    here = jnp.where(is_odd, passed[0], 0.0)
    to_near = back_even[0] + jnp.where(is_odd, passed[1], passed[0])
    to_far = back_even[1] + jnp.where(is_odd, 0.0, passed[1])
    returns = around(to_near, 2) + around(to_far, 4) + here
    returns = returns.reshape(-1, tile_count, tile_len)
    total = gained_same + gained_ahead + returns[0]
    if two:
        total = total + lax.ppermute(returns[1], "wall", swap)
    else:
        total = total + from_wall(returns[2], 1) + from_wall(returns[1], -1)
    return (total * filled * (1.0 / (math.pi * NB * tile_len))).reshape(1, 1, -1)


def solution(mesh):
    placed = (
        P(None, "chan", "wall", None),
        P("chan", "wall", None),
        P("chan", "wall", None),
        P("chan", "wall", None, None, None),
    )
    return jax.shard_map(
        on_device, mesh=mesh, in_specs=placed, out_specs=P("chan", "wall", None), check_vma=False
    )
```
